32 devices in a mesh: gz: 32 (over z, y, x, core).
Axes of the slice: x: 2, y: 2, z: 4, core: 2. Of those that a mesh axis runs over, the one named last changes fastest.
Arguments:
- scores: int32 [128, 512, 512], P('gz'), may hold values from 0 to 33554431, as said below
Outputs:
- status: int32 [128, 512, 512], P('gz')
- counts: int32 [3], replicated
The draws below stay inside these ranges and needn't reach their ends.
Inputs may be any that keep to these rules, and one draw needn't show every extreme that they name: `scores`: all values distinct: a permutation of 0 to 33554431.
All inputs are finite; a program needn't handle non-finite values.
Results may differ from the reference program's by a relative error of at most 0.000001.
Values may be sent and summed in bfloat16 or wider, within the bound.
A program may use at most 64 MiB of HBM per device.

```python
import jax
import jax.numpy as jnp

NX = 512
NY = 512
ROUNDS = 3
NZ = 128


def draw_scores(key, part):
    return jax.random.permutation(key, NX * NY * NZ).astype(jnp.int32).reshape(NZ, NX, NY)


def setup_inputs(seed: int = 0) -> dict:
    splits = jax.random.split(jax.random.key(seed), 2)
    return {
        "scores": draw_scores(jax.random.fold_in(splits[1], 71), 0),
    }


ceiling = 1 << 30


def lateral_max(field):
    padded = jnp.pad(field, ((0, 0), (1, 1), (1, 1)))
    rows_max = jnp.maximum(jnp.maximum(padded[:, :-2, :], padded[:, 1:-1, :]), padded[:, 2:, :])
    return jnp.maximum(jnp.maximum(rows_max[:, :, :-2], rows_max[:, :, 1:-1]), rows_max[:, :, 2:])


def box_maximum(extended):
    depth_max = jnp.maximum(jnp.maximum(extended[:-2], extended[1:-1]), extended[2:])
    return lateral_max(depth_max)


def reference(scores):
    status = jnp.zeros(scores.shape, jnp.int32)
    totals = []
    for round_index in range(ROUNDS):
        labels = jnp.where(status == 0, 4 * scores + 4, jnp.where(status == 1, ceiling, 0)).astype(jnp.int32)
        near_max = box_maximum(jnp.pad(labels, ((1, 1), (0, 0), (0, 0))))
        far_max = box_maximum(jnp.pad(near_max, ((1, 1), (0, 0), (0, 0))))
        undecided = status == 0
        status = jnp.where(undecided & (far_max >= ceiling), 2,
                           jnp.where(undecided & (far_max == labels), 1, status)).astype(jnp.int32)
        totals.append(jnp.sum((status == 0).astype(jnp.int32)).astype(jnp.int32))
    return status, jnp.stack(totals).astype(jnp.int32)
```

```python
import functools

import jax
import jax.numpy as jnp
from jax import lax
from jax.experimental import pallas as pl
from jax.experimental.pallas import tpu as pltpu
from jax.sharding import PartitionSpec as P


AXIS = "gz"
ROWS = 32
PAD = 8


def shifted(x, shift, axis):
    return pltpu.roll(x, shift % x.shape[axis], axis)


def spread(x, op, blank, lane):
    pair = op(x, shifted(x, -1, 0))
    x = op(op(pair, shifted(pair, 2, 0)), shifted(x, -2, 0))[PAD:-PAD]
    ny = x.shape[1]
    after = shifted(x, -1, 1)
    pair = op(jnp.where(lane >= ny - 1, blank, x), after)
    return op(
        op(
            op(x, jnp.where(lane >= ny - 1, blank, after)),
            jnp.where(lane < 1, blank, shifted(pair, 2, 1)),
        ),
        jnp.where(lane >= ny - 2, blank, shifted(x, -2, 1)),
    )


def pack(x):
    half = x.shape[1] // 2
    row = lax.broadcasted_iota(jnp.int32, (8, half), 0) % 2 == 0
    lane = lax.broadcasted_iota(jnp.int32, (8, half), 1) % 2 == 0
    out = []
    for r in range(0, x.shape[0], 16):
        quads = []
        for part in (x[r : r + 8], x[r + 8 : r + 16]):
            part = jnp.maximum(part, shifted(part, -1, 0))
            part = jnp.maximum(part, shifted(part, -1, 1))
            quads.append(jnp.where(lane, part[:, :half], shifted(part[:, half:], 1, 1)))
        out.append(jnp.where(row, quads[0], shifted(quads[1], 1, 0)))
    return jnp.concatenate(out, axis=0)


def unpack(x):
    half = x.shape[1]
    row = lax.broadcasted_iota(jnp.int32, (8, half), 0) % 2 == 0
    lane = lax.broadcasted_iota(jnp.int32, (8, half), 1) % 2 == 0
    out = []
    for r in range(0, x.shape[0], 8):
        part = x[r : r + 8]
        for rows in (
            jnp.where(row, part, shifted(part, 1, 0)),
            jnp.where(row, shifted(part, -1, 0), part),
        ):
            out.append(
                jnp.concatenate(
                    [
                        jnp.where(lane, rows, shifted(rows, 1, 1)),
                        jnp.where(lane, shifted(rows, -1, 1), rows),
                    ],
                    axis=1,
                )
            )
    return jnp.concatenate(out, axis=0)


def kernel(
    n, scores, packed_status, counts, field, near, bits, found, cand_send, cand_recv,
    resp_send, resp_recv, tally, cnt_send, cnt_recv, in_sem, send_sem, recv_sem,
    cnt_send_sem, cnt_recv_sem,
):
    depth, nx, ny = scores.shape
    me = lax.axis_index(AXIS)
    has = (me > 0, me < n - 1)
    lone = tuple(jnp.where(h, 0, 1).astype(jnp.int32) for h in has)
    edge = ((0, 1), (depth - 2, depth - 1))
    halo_bits = ((0, 1), (depth + 2, depth + 3))
    lane = lax.broadcasted_iota(jnp.int32, (ROWS, ny), 1)
    spot = (lax.broadcasted_iota(jnp.int32, (ROWS, ny), 0) % 2) * 2 + lane % 2
    blocks = nx // ROWS

    load = pltpu.make_async_copy(scores, field.at[:, pl.ds(PAD, nx), :], in_sem)
    load.start()
    for rows in (slice(0, PAD), slice(PAD + nx, 2 * PAD + nx)):
        field[:, rows, :] = jnp.full((depth, PAD, ny), -1, jnp.int32)
        bits[rows, :] = jnp.zeros((PAD, ny), jnp.int32)
    tally[...] = jnp.zeros_like(tally)
    for side in range(2):

        @pl.when(jnp.logical_not(has[side]))
        def _():
            for phase in range(2):
                cand_recv[phase, side] = jnp.full(cand_recv.shape[2:], -1, jnp.int32)
                resp_recv[phase, side] = jnp.ones(resp_recv.shape[2:], jnp.bfloat16)

    load.wait()

    def exchange(send, recv, phase, step, side):
        return pltpu.make_async_remote_copy(
            src_ref=send.at[phase, side],
            dst_ref=recv.at[phase, 1 - side],
            send_sem=send_sem.at[step, side],
            recv_sem=recv_sem.at[step, 1 - side],
            device_id=(me + (1 if side else -1),),
            device_id_type=pl.DeviceIdType.MESH,
        )

    def start(send, recv, phase, step):
        for side in range(2):

            @pl.when(has[side])
            def _():
                exchange(send, recv, phase, step, side).start()

    def finish(send, recv, phase, step):
        for side in range(2):

            @pl.when(has[side])
            def _():
                copy = exchange(send, recv, phase, step, side)
                copy.wait_send()
                pltpu.make_async_remote_copy(
                    src_ref=send.at[phase, side],
                    dst_ref=recv.at[phase, side],
                    send_sem=send_sem.at[step, side],
                    recv_sem=recv_sem.at[step, side],
                    device_id=(me + (1 if side else -1),),
                    device_id_type=pl.DeviceIdType.MESH,
                ).wait_recv()

    def search(phase):
        @pl.loop(0, blocks)
        def _(block):
            top = pl.multiple_of(block * ROWS, ROWS)
            centre = pl.ds(pl.multiple_of(top + PAD, PAD), ROWS)
            wide = [
                spread(field[z, pl.ds(top, ROWS + 2 * PAD), :], jnp.maximum, -1, lane)
                for z in range(depth)
            ]
            near[0, 0, pl.ds(top, ROWS), :] = wide[0]
            near[0, 1, pl.ds(top, ROWS), :] = jnp.maximum(wide[0], wide[1])
            near[1, 0, pl.ds(top, ROWS), :] = jnp.maximum(wide[-1], wide[-2])
            near[1, 1, pl.ds(top, ROWS), :] = wide[-1]
            own = jnp.zeros((ROWS, ny), jnp.int32)
            best, held = [], []
            for z in range(depth):
                value = field[z, centre, :]
                peak = functools.reduce(
                    jnp.maximum, wide[max(z - 2, 0) : min(z + 3, depth)]
                )
                is_best = value == peak
                if phase:
                    is_best = is_best & (value >= 0)
                own = own | jnp.where(is_best, 4 << z, 0)
                best.append(is_best)
                held.append(value)
            found[pl.ds(top, ROWS), :] = own
            for side in range(2):
                low, high = edge[side]
                code = jnp.where(
                    best[low],
                    held[low] * 8 + spot,
                    jnp.where(best[high], held[high] * 8 + (spot + 4), -1),
                )
                cand_send[phase, side, pl.ds(pl.multiple_of(top // 2, ROWS // 2), ROWS // 2), :] = pack(code)
            if phase:
                total = tally[2]
                for side in range(2):
                    for z in edge[side]:
                        total = total + jnp.where(best[z], lone[side], 0)
                for z in range(2, depth - 2):
                    total = total + jnp.where(best[z], 1, 0)
                tally[2] = total

    def judge(phase):
        @pl.loop(0, blocks)
        def _(block):
            top = pl.multiple_of(block * ROWS, ROWS)
            small = pl.ds(pl.multiple_of(block * (ROWS // 2), ROWS // 2), ROWS // 2)
            halo = jnp.zeros((ROWS, ny), jnp.int32)
            for side in range(2):
                code = unpack(cand_recv[phase, side, small, :])
                place, score = code & 7, code >> 3
                low = (place == spot) & (score > near[side, 0, pl.ds(top, ROWS), :])
                high = (place == spot + 4) & (score > near[side, 1, pl.ds(top, ROWS), :])
                alive = jnp.where(low | high, 1, 0)
                resp_send[phase, side, small, :] = (
                    pack(alive).astype(jnp.float32).astype(jnp.bfloat16)
                )
                if phase:
                    tally[2] += alive
                else:
                    halo = halo | jnp.where(low, 1 << halo_bits[side][0], 0)
                    halo = halo | jnp.where(high, 1 << halo_bits[side][1], 0)
            if not phase:
                bits[pl.ds(pl.multiple_of(top + PAD, PAD), ROWS), :] = halo

    def confirmed(phase, block):
        top = pl.multiple_of(block * ROWS, ROWS)
        small = pl.ds(pl.multiple_of(block * (ROWS // 2), ROWS // 2), ROWS // 2)
        own = found[pl.ds(top, ROWS), :]
        for side in range(2):
            alive = unpack(resp_recv[phase, side, small, :].astype(jnp.float32))
            mask = (4 << edge[side][0]) | (4 << edge[side][1])
            own = jnp.where(alive > 0.5, own, own & ~mask)
        return own

    search(0)
    start(cand_send, cand_recv, 0, 0)
    finish(cand_send, cand_recv, 0, 0)
    judge(0)
    start(resp_send, resp_recv, 0, 1)
    finish(resp_send, resp_recv, 0, 1)

    @pl.loop(0, blocks)
    def _(block):
        bits[pl.ds(pl.multiple_of(block * ROWS + PAD, PAD), ROWS), :] |= confirmed(0, block)

    @pl.loop(0, blocks)
    def _(block):
        top = pl.multiple_of(block * ROWS, ROWS)
        centre = pl.ds(pl.multiple_of(top + PAD, PAD), ROWS)
        roots = bits[centre, :]
        reach = spread(bits[pl.ds(top, ROWS + 2 * PAD), :], jnp.bitwise_or, 0, lane)
        status = jnp.zeros((ROWS, ny), jnp.int32)
        first, second = tally[0], tally[1]
        for z in range(depth):
            is_root = (roots & (4 << z)) != 0
            covered = (reach & (31 << z)) != 0
            field[z, centre, :] = jnp.where(covered, -1, field[z, centre, :])
            status = status | jnp.where(
                is_root, 1 << (2 * z), jnp.where(covered, 2 << (2 * z), 0)
            )
            first = first + jnp.where(is_root, 1, 0)
            second = second + jnp.where(covered, 1, 0)
        tally[0] = first
        tally[1] = second
        packed_status[pl.ds(top, ROWS), :] = status

    search(1)
    start(cand_send, cand_recv, 1, 2)
    finish(cand_send, cand_recv, 1, 2)
    judge(1)
    start(resp_send, resp_recv, 1, 3)

    roots, covered, late = (jnp.sum(tally[i]) for i in range(3))
    cells = depth * nx * ny
    column = lax.broadcasted_iota(jnp.int32, cnt_send.shape, 1)
    mine = jnp.where(
        column == 0,
        cells - roots,
        jnp.where(column == 1, cells - covered, cells - covered - late),
    )
    cnt_send[...] = mine

    def report(i):
        return pltpu.make_async_remote_copy(
            src_ref=cnt_send,
            dst_ref=cnt_recv.at[i],
            send_sem=cnt_send_sem.at[i],
            recv_sem=cnt_recv_sem.at[i],
            device_id=(lax.rem(me + i, n),),
            device_id_type=pl.DeviceIdType.MESH,
        )

    @pl.loop(1, n)
    def _(i):
        report(i).start()

    finish(resp_send, resp_recv, 1, 3)

    @pl.loop(0, blocks)
    def _(block):
        own = confirmed(1, block)
        rows = pl.ds(pl.multiple_of(block * ROWS, ROWS), ROWS)
        status = packed_status[rows, :]
        for z in range(depth):
            status = status | jnp.where((own & (4 << z)) != 0, 1 << (2 * z), 0)
        packed_status[rows, :] = status

    @pl.loop(1, n)
    def _(i):
        report(i).wait()

    cnt_recv[0] = mine
    counts[...] = jnp.sum(cnt_recv[...], axis=0)


def shards(scores):
    depth, nx, ny = scores.shape
    n = lax.axis_size(AXIS)
    vmem = pltpu.VMEM
    small = (nx // 2, ny // 2)
    packed_status, counts = pl.pallas_call(
        functools.partial(kernel, n),
        out_shape=(
            jax.ShapeDtypeStruct((nx, ny), jnp.int32),
            jax.ShapeDtypeStruct((8, 128), jnp.int32),
        ),
        in_specs=[pl.BlockSpec(memory_space=pl.ANY)],
        out_specs=(pl.BlockSpec(memory_space=vmem),) * 2,
        scratch_shapes=[
            vmem((depth, nx + 2 * PAD, ny), jnp.int32),
            vmem((2, 2, nx, ny), jnp.int32),
            vmem((nx + 2 * PAD, ny), jnp.int32),
            vmem((nx, ny), jnp.int32),
            vmem((2, 2) + small, jnp.int32),
            vmem((2, 2) + small, jnp.int32),
            vmem((2, 2) + small, jnp.bfloat16),
            vmem((2, 2) + small, jnp.bfloat16),
            vmem((3, ROWS, ny), jnp.int32),
            vmem((8, 128), jnp.int32),
            vmem((n, 8, 128), jnp.int32),
            pltpu.SemaphoreType.DMA,
            pltpu.SemaphoreType.DMA((4, 2)),
            pltpu.SemaphoreType.DMA((4, 2)),
            pltpu.SemaphoreType.DMA((n,)),
            pltpu.SemaphoreType.DMA((n,)),
        ],
        compiler_params=pltpu.CompilerParams(
            has_side_effects=True, vmem_limit_bytes=48 * 1024 * 1024
        ),
    )(scores)
    place = 2 * jnp.arange(depth, dtype=jnp.int32)[:, None, None]
    return (packed_status[None] >> place) & 3, counts[0, :3]


def solution(mesh):
    return jax.shard_map(
        shards,
        mesh=mesh,
        in_specs=(P(AXIS, None, None),),
        out_specs=(P(AXIS, None, None), P()),
        check_vma=False,
    )
```

```python
import functools

import jax
import jax.numpy as jnp
from jax import lax
from jax.experimental import pallas as pl
from jax.experimental.pallas import tpu as pltpu
from jax.sharding import PartitionSpec as P


AXIS = "gz"
FINE = 16
ROWS = 32
PARTS = 4
PAD = 8
LANES = 128
NONE = -(2.0**126)


def roll(x, shift, axis):
    return pltpu.roll(x, shift % x.shape[axis], axis)


def encode(score, total):
    if total <= 1 << 25:
        return (score - (1 << 24)).astype(jnp.float32)
    value = ((score & ((1 << 23) - 1)) + (1 << 23)).astype(jnp.float32)
    for bit in range(23, (total - 1).bit_length()):
        factor = jnp.where((score & (1 << bit)) != 0, 2.0 ** (1 << (bit - 23)), 1.0)
        value = value * factor
    return value


def spread(load, chunks, op, blank, lane):
    x = [
        op(
            op(op(load(c, -2), load(c, -1)), op(load(c, 0), load(c, 1))),
            load(c, 2),
        )
        for c in range(chunks)
    ]
    one = [roll(v, -1, 1) for v in x] + [blank]
    two = [roll(v, -2, 1) for v in x] + [blank]
    pair = [
        op(x[c], jnp.where(lane >= LANES - 1, one[c + 1], one[c])) for c in range(chunks)
    ]
    before = [jnp.where(lane == 1, roll(x[0], 1, 1), blank)]
    before += [roll(v, 2, 1) for v in pair]
    return [
        op(
            op(pair[c], jnp.where(lane < 2, before[c], before[c + 1])),
            jnp.where(lane >= LANES - 2, two[c + 1], two[c]),
        )
        for c in range(chunks)
    ]


def parity():
    row = lax.broadcasted_iota(jnp.int32, (8, LANES), 0) % 2 == 0
    lane = lax.broadcasted_iota(jnp.int32, (8, LANES), 1) % 2 == 0
    return row, lane


def pack(x):
    row, lane = parity()
    half = len(x) // 2

    def fold(part):
        part = jnp.maximum(part, roll(part, -1, 0))
        return jnp.maximum(part, roll(part, -1, 1))

    out = []
    for c in range(half):
        rows = []
        for r in range(0, x[0].shape[0], 16):
            quads = [
                jnp.where(
                    lane, fold(x[c][k : k + 8]), roll(fold(x[c + half][k : k + 8]), 1, 1)
                )
                for k in (r, r + 8)
            ]
            rows.append(jnp.where(row, quads[0], roll(quads[1], 1, 0)))
        out.append(jnp.concatenate(rows, axis=0))
    return out


def unpack(x):
    row, lane = parity()
    low, high = [], []
    for v in x:
        lows, highs = [], []
        for r in range(0, v.shape[0], 8):
            part = v[r : r + 8]
            for rows in (
                jnp.where(row, part, roll(part, 1, 0)),
                jnp.where(row, roll(part, -1, 0), part),
            ):
                lows.append(jnp.where(lane, rows, roll(rows, 1, 1)))
                highs.append(jnp.where(lane, roll(rows, -1, 1), rows))
        low.append(jnp.concatenate(lows, axis=0))
        high.append(jnp.concatenate(highs, axis=0))
    return low + high


def kernel(
    n, scores, packed_status, counts, field, near, bits, found, cand_send, cand_recv,
    resp_send, resp_recv, tally, cnt_send, cnt_recv, send_sem, recv_sem,
    cnt_send_sem, cnt_recv_sem,
):
    depth, nx, ny = scores.shape
    total = n * depth * nx * ny
    chunks = ny // LANES
    me = lax.axis_index(AXIS)
    has = (me > 0, me < n - 1)
    lone = tuple(jnp.where(h, 0, 1).astype(jnp.int32) for h in has)
    edge = ((0, 1), (depth - 2, depth - 1))
    halo_bits = ((0, 1), (depth + 2, depth + 3))
    lane = lax.broadcasted_iota(jnp.int32, (FINE, LANES), 1)

    def spot(rows):
        shape = (rows, LANES)
        row = lax.broadcasted_iota(jnp.int32, shape, 0) % 2
        return row * 2 + lax.broadcasted_iota(jnp.int32, shape, 1) % 2

    part_rows = nx // PARTS
    columns = [slice(c * LANES, (c + 1) * LANES) for c in range(chunks)]

    barrier = pltpu.get_barrier_semaphore()

    @pl.loop(1, n)
    def _(i):
        pl.semaphore_signal(
            barrier,
            inc=1,
            device_id=(lax.rem(me + i, n),),
            device_id_type=pl.DeviceIdType.MESH,
        )

    for rows in (slice(0, PAD), slice(PAD + nx, 2 * PAD + nx)):
        field[:, :, rows, :] = jnp.full((depth, chunks, PAD, LANES), NONE, jnp.float32)
        bits[:, rows, :] = jnp.zeros((chunks, PAD, LANES), jnp.int32)
    tally[...] = jnp.zeros_like(tally)
    for side in range(2):

        @pl.when(jnp.logical_not(has[side]))
        def _():
            for phase in range(2):
                cand_recv[phase, side] = jnp.full(cand_recv.shape[2:], -1, jnp.int32)
                resp_recv[phase, side] = jnp.ones(resp_recv.shape[2:], jnp.bfloat16)

    @pl.loop(0, nx // ROWS)
    def _(block):
        top = pl.multiple_of(block * ROWS, ROWS)
        for z in range(depth):
            for c in range(chunks):
                field[z, c, pl.ds(pl.multiple_of(top + PAD, PAD), ROWS), :] = encode(
                    scores[z, pl.ds(top, ROWS), columns[c]], total
                )

    pl.semaphore_wait(barrier, n - 1)

    def exchange(send, recv, phase, step, side, part, arrival):
        rows = pl.ds(pl.multiple_of(part * (part_rows // 2), part_rows // 2), part_rows // 2)
        there = arrival if arrival is not None else 1 - side
        return pltpu.make_async_remote_copy(
            src_ref=send.at[phase, side, rows, :],
            dst_ref=recv.at[phase, there, rows, :],
            send_sem=send_sem.at[step, side, part],
            recv_sem=recv_sem.at[step, there, part],
            device_id=(me + (1 if side else -1),),
            device_id_type=pl.DeviceIdType.MESH,
        )

    def start(send, recv, phase, step, part):
        for side in range(2):

            @pl.when(has[side])
            def _():
                exchange(send, recv, phase, step, side, part, None).start()

    def finish(send, recv, phase, step, part):
        for side in range(2):

            @pl.when(has[side])
            def _():
                exchange(send, recv, phase, step, side, part, None).wait_send()
                exchange(send, recv, phase, step, side, part, side).wait_recv()

    def search(phase, part):
        place = spot(FINE)

        @pl.loop(0, part_rows // FINE)
        def _(block):
            top = pl.multiple_of(part * part_rows + block * FINE, FINE)
            here = pl.ds(top, FINE)
            wide = [
                spread(
                    lambda c, d: field[z, c, pl.ds(top + (PAD + d), FINE), :],
                    chunks, jnp.maximum, NONE, lane,
                )
                for z in range(depth)
            ]
            codes = ([], [])
            count = jnp.zeros((FINE, LANES), jnp.int32)
            for c in range(chunks):
                w = [wide[z][c] for z in range(depth)]
                low, high = jnp.maximum(w[0], w[1]), jnp.maximum(w[-1], w[-2])
                near[0, 0, c, here, :] = w[0]
                near[0, 1, c, here, :] = low
                near[1, 0, c, here, :] = high
                near[1, 1, c, here, :] = w[-1]
                own = jnp.zeros((FINE, LANES), jnp.int32)
                best = []
                for z in range(depth):
                    value = field[z, c, pl.ds(pl.multiple_of(top + PAD, PAD), FINE), :]
                    terms = {k: w[k] for k in range(max(z - 2, 0), min(z + 3, depth))}
                    if 0 in terms and 1 in terms:
                        terms[0] = low
                        del terms[1]
                    if depth - 1 in terms and depth - 2 in terms:
                        terms[depth - 1] = high
                        del terms[depth - 2]
                    is_best = value == functools.reduce(jnp.maximum, list(terms.values()))
                    if phase:
                        is_best = is_best & (value > NONE)
                    own = own | jnp.where(is_best, 4 << z, 0)
                    best.append(is_best)
                found[c, here, :] = own
                for side in range(2):
                    a, b = edge[side]
                    held_a = scores[a, here, columns[c]]
                    held_b = scores[b, here, columns[c]]
                    codes[side].append(
                        jnp.where(
                            best[a],
                            held_a * 8 + place,
                            jnp.where(best[b], held_b * 8 + (place + 4), -1),
                        )
                    )
                if phase:
                    for side in range(2):
                        for z in edge[side]:
                            count = count + jnp.where(best[z], lone[side], 0)
                    for z in range(2, depth - 2):
                        count = count + jnp.where(best[z], 1, 0)
            small = pl.ds(pl.multiple_of(top // 2, FINE // 2), FINE // 2)
            for side in range(2):
                for c, v in enumerate(pack(codes[side])):
                    cand_send[phase, side, small, columns[c]] = v
            if phase:
                tally[2, :FINE] += count

    def judge(phase, part):
        place = spot(ROWS)

        @pl.loop(0, part_rows // ROWS)
        def _(block):
            top = pl.multiple_of(part * part_rows + block * ROWS, ROWS)
            small = pl.ds(pl.multiple_of(top // 2, ROWS // 2), ROWS // 2)
            here = pl.ds(top, ROWS)
            halo = [jnp.zeros((ROWS, LANES), jnp.int32) for _ in range(chunks)]
            count = jnp.zeros((ROWS, LANES), jnp.int32)
            for side in range(2):
                codes = unpack(
                    [cand_recv[phase, side, small, columns[c]] for c in range(chunks // 2)]
                )
                verdicts = []
                for c, code in enumerate(codes):
                    where = code & 7
                    score = jnp.where(code < 0, NONE, encode(code >> 3, total))
                    low = (where == place) & (score > near[side, 0, c, here, :])
                    high = (where == place + 4) & (score > near[side, 1, c, here, :])
                    alive = jnp.where(low | high, 1, 0)
                    verdicts.append(alive)
                    if phase:
                        count = count + alive
                    else:
                        halo[c] = halo[c] | jnp.where(low, 1 << halo_bits[side][0], 0)
                        halo[c] = halo[c] | jnp.where(high, 1 << halo_bits[side][1], 0)
                for c, v in enumerate(pack(verdicts)):
                    resp_send[phase, side, small, columns[c]] = v.astype(
                        jnp.float32
                    ).astype(jnp.bfloat16)
            if phase:
                tally[2] += count
            else:
                for c in range(chunks):
                    bits[c, pl.ds(pl.multiple_of(top + PAD, PAD), ROWS), :] = halo[c]

    def confirmed(phase, top):
        small = pl.ds(pl.multiple_of(top // 2, ROWS // 2), ROWS // 2)
        own = [found[c, pl.ds(top, ROWS), :] for c in range(chunks)]
        for side in range(2):
            verdicts = unpack(
                [
                    resp_recv[phase, side, small, columns[c]].astype(jnp.float32)
                    for c in range(chunks // 2)
                ]
            )
            mask = (4 << edge[side][0]) | (4 << edge[side][1])
            own = [jnp.where(v > 0.5, o, o & ~mask) for v, o in zip(verdicts, own)]
        return own

    def settle(part):
        @pl.loop(0, part_rows // ROWS)
        def _(block):
            top = pl.multiple_of(part * part_rows + block * ROWS, ROWS)
            for c, own in enumerate(confirmed(0, top)):
                bits[c, pl.ds(pl.multiple_of(top + PAD, PAD), ROWS), :] |= own

    def remove(part):
        @pl.loop(0, part_rows // FINE)
        def _(block):
            top = pl.multiple_of(part * part_rows + block * FINE, FINE)
            centre = pl.ds(pl.multiple_of(top + PAD, PAD), FINE)
            reach = spread(
                lambda c, d: bits[c, pl.ds(top + (PAD + d), FINE), :],
                chunks, jnp.bitwise_or, 0, lane,
            )
            first, second = tally[0, :FINE], tally[1, :FINE]
            for c in range(chunks):
                roots = bits[c, centre, :]
                status = jnp.zeros((FINE, LANES), jnp.int32)
                for z in range(depth):
                    is_root = (roots & (4 << z)) != 0
                    covered = (reach[c] & (31 << z)) != 0
                    field[z, c, centre, :] = jnp.where(covered, NONE, field[z, c, centre, :])
                    status = status | jnp.where(
                        is_root, 1 << (2 * z), jnp.where(covered, 2 << (2 * z), 0)
                    )
                    first = first + jnp.where(is_root, 1, 0)
                    second = second + jnp.where(covered, 1, 0)
                packed_status[pl.ds(top, FINE), columns[c]] = status
            tally[0, :FINE] = first
            tally[1, :FINE] = second

    for phase in range(2):

        @pl.loop(0, PARTS)
        def _(part):
            search(phase, part)
            start(cand_send, cand_recv, phase, 2 * phase, part)

        @pl.loop(0, PARTS)
        def _(part):
            finish(cand_send, cand_recv, phase, 2 * phase, part)
            judge(phase, part)
            start(resp_send, resp_recv, phase, 2 * phase + 1, part)

        if phase == 0:

            @pl.loop(0, PARTS)
            def _(part):
                finish(resp_send, resp_recv, 0, 1, part)
                settle(part)

                @pl.when(part > 0)
                def _():
                    remove(part - 1)

            remove(PARTS - 1)

    roots, covered, late = (jnp.sum(tally[i]) for i in range(3))
    cells = depth * nx * ny
    column = lax.broadcasted_iota(jnp.int32, cnt_send.shape, 1)
    mine = jnp.where(
        column == 0,
        cells - roots,
        jnp.where(column == 1, cells - covered, cells - covered - late),
    )
    cnt_send[...] = mine

    def report(i):
        return pltpu.make_async_remote_copy(
            src_ref=cnt_send,
            dst_ref=cnt_recv.at[i],
            send_sem=cnt_send_sem.at[i],
            recv_sem=cnt_recv_sem.at[i],
            device_id=(lax.rem(me + i, n),),
            device_id_type=pl.DeviceIdType.MESH,
        )

    @pl.loop(1, n)
    def _(i):
        report(i).start()

    @pl.loop(0, PARTS)
    def _(part):
        finish(resp_send, resp_recv, 1, 3, part)

        @pl.loop(0, part_rows // ROWS)
        def _(block):
            top = pl.multiple_of(part * part_rows + block * ROWS, ROWS)
            for c, own in enumerate(confirmed(1, top)):
                status = packed_status[pl.ds(top, ROWS), columns[c]]
                for z in range(depth):
                    status = status | jnp.where((own & (4 << z)) != 0, 1 << (2 * z), 0)
                packed_status[pl.ds(top, ROWS), columns[c]] = status

    @pl.loop(1, n)
    def _(i):
        report(i).wait()

    cnt_recv[0] = mine
    counts[...] = jnp.sum(cnt_recv[...], axis=0)


def shards(scores):
    depth, nx, ny = scores.shape
    n = lax.axis_size(AXIS)
    vmem = pltpu.VMEM
    small = (nx // 2, ny // 2)
    chunks = ny // LANES
    packed_status, counts = pl.pallas_call(
        functools.partial(kernel, n),
        out_shape=(
            jax.ShapeDtypeStruct((nx, ny), jnp.int32),
            jax.ShapeDtypeStruct((8, 128), jnp.int32),
        ),
        in_specs=[pl.BlockSpec(memory_space=vmem)],
        out_specs=(pl.BlockSpec(memory_space=vmem),) * 2,
        scratch_shapes=[
            vmem((depth, chunks, nx + 2 * PAD, LANES), jnp.float32),
            vmem((2, 2, chunks, nx, LANES), jnp.float32),
            vmem((chunks, nx + 2 * PAD, LANES), jnp.int32),
            vmem((chunks, nx, LANES), jnp.int32),
            vmem((2, 2) + small, jnp.int32),
            vmem((2, 2) + small, jnp.int32),
            vmem((2, 2) + small, jnp.bfloat16),
            vmem((2, 2) + small, jnp.bfloat16),
            vmem((3, ROWS, LANES), jnp.int32),
            vmem((8, 128), jnp.int32),
            vmem((n, 8, 128), jnp.int32),
            pltpu.SemaphoreType.DMA((4, 2, PARTS)),
            pltpu.SemaphoreType.DMA((4, 2, PARTS)),
            pltpu.SemaphoreType.DMA((n,)),
            pltpu.SemaphoreType.DMA((n,)),
        ],
        compiler_params=pltpu.CompilerParams(
            collective_id=0, has_side_effects=True, vmem_limit_bytes=48 * 1024 * 1024
        ),
    )(scores)
    place = 2 * jnp.arange(depth, dtype=jnp.int32)[:, None, None]
    return (packed_status[None] >> place) & 3, counts[0, :3]


def solution(mesh):
    return jax.shard_map(
        shards,
        mesh=mesh,
        in_specs=(P(AXIS, None, None),),
        out_specs=(P(AXIS, None, None), P()),
        check_vma=False,
    )
```

```python
import functools

import jax
import jax.numpy as jnp
from jax import lax
from jax.experimental import pallas as pl
from jax.experimental.pallas import tpu as pltpu
from jax.sharding import PartitionSpec as P


AXIS = "gz"
FINE = 32
ROWS = 64
PARTS = 4
PAD = 8
LANES = 128
NONE = -(2.0**126)


def roll(x, shift, axis):
    return pltpu.roll(x, shift % x.shape[axis], axis)


def encode(score, total):
    if total <= 1 << 25:
        return (score - (1 << 24)).astype(jnp.float32)
    value = ((score & ((1 << 23) - 1)) + (1 << 23)).astype(jnp.float32)
    for bit in range(23, (total - 1).bit_length()):
        factor = jnp.where((score & (1 << bit)) != 0, 2.0 ** (1 << (bit - 23)), 1.0)
        value = value * factor
    return value


def spread(load, chunks, op, blank, lane):
    x = [
        op(
            op(op(load(c, -2), load(c, -1)), op(load(c, 0), load(c, 1))),
            load(c, 2),
        )
        for c in range(chunks)
    ]
    one = [roll(v, -1, 1) for v in x] + [blank]
    two = [roll(v, -2, 1) for v in x] + [blank]
    pair = [
        op(x[c], jnp.where(lane >= LANES - 1, one[c + 1], one[c])) for c in range(chunks)
    ]
    before = [jnp.where(lane == 1, roll(x[0], 1, 1), blank)]
    before += [roll(v, 2, 1) for v in pair]
    return [
        op(
            op(pair[c], jnp.where(lane < 2, before[c], before[c + 1])),
            jnp.where(lane >= LANES - 2, two[c + 1], two[c]),
        )
        for c in range(chunks)
    ]


def parity():
    row = lax.broadcasted_iota(jnp.int32, (8, LANES), 0) % 2 == 0
    lane = lax.broadcasted_iota(jnp.int32, (8, LANES), 1) % 2 == 0
    return row, lane


def pack(x):
    row, lane = parity()
    half = len(x) // 2

    def fold(part):
        part = jnp.maximum(part, roll(part, -1, 0))
        return jnp.maximum(part, roll(part, -1, 1))

    out = []
    for c in range(half):
        rows = []
        for r in range(0, x[0].shape[0], 16):
            quads = [
                jnp.where(
                    lane, fold(x[c][k : k + 8]), roll(fold(x[c + half][k : k + 8]), 1, 1)
                )
                for k in (r, r + 8)
            ]
            rows.append(jnp.where(row, quads[0], roll(quads[1], 1, 0)))
        out.append(jnp.concatenate(rows, axis=0))
    return out


def unpack(x):
    row, lane = parity()
    low, high = [], []
    for v in x:
        lows, highs = [], []
        for r in range(0, v.shape[0], 8):
            part = v[r : r + 8]
            for rows in (
                jnp.where(row, part, roll(part, 1, 0)),
                jnp.where(row, roll(part, -1, 0), part),
            ):
                lows.append(jnp.where(lane, rows, roll(rows, 1, 1)))
                highs.append(jnp.where(lane, roll(rows, -1, 1), rows))
        low.append(jnp.concatenate(lows, axis=0))
        high.append(jnp.concatenate(highs, axis=0))
    return low + high


def kernel(
    n, scores, packed_status, counts, field, near, bits, found, cand_send, cand_recv,
    resp_send, resp_recv, tally, cnt_send, cnt_recv, send_sem, recv_sem,
    cnt_send_sem, cnt_recv_sem,
):
    depth, nx, ny = scores.shape
    total = n * depth * nx * ny
    chunks = ny // LANES
    me = lax.axis_index(AXIS)
    has = (me > 0, me < n - 1)
    lone = tuple(jnp.where(h, 0, 1).astype(jnp.int32) for h in has)
    edge = ((0, 1), (depth - 2, depth - 1))
    halo_bits = ((0, 1), (depth + 2, depth + 3))
    lane = lax.broadcasted_iota(jnp.int32, (FINE, LANES), 1)

    def spot(rows):
        shape = (rows, LANES)
        row = lax.broadcasted_iota(jnp.int32, shape, 0) % 2
        return row * 2 + lax.broadcasted_iota(jnp.int32, shape, 1) % 2

    part_rows = nx // PARTS
    columns = [slice(c * LANES, (c + 1) * LANES) for c in range(chunks)]

    barrier = pltpu.get_barrier_semaphore()

    @pl.loop(1, n)
    def _(i):
        pl.semaphore_signal(
            barrier,
            inc=1,
            device_id=(lax.rem(me + i, n),),
            device_id_type=pl.DeviceIdType.MESH,
        )

    for rows in (slice(0, PAD), slice(PAD + nx, 2 * PAD + nx)):
        field[:, :, rows, :] = jnp.full((depth, chunks, PAD, LANES), NONE, jnp.float32)
        bits[:, rows, :] = jnp.zeros((chunks, PAD, LANES), jnp.int32)
    tally[...] = jnp.zeros_like(tally)
    for side in range(2):

        @pl.when(jnp.logical_not(has[side]))
        def _():
            for phase in range(2):
                cand_recv[phase, side] = jnp.full(cand_recv.shape[2:], -1, jnp.int32)
                resp_recv[phase, side] = jnp.ones(resp_recv.shape[2:], jnp.bfloat16)

    @pl.loop(0, nx // ROWS)
    def _(block):
        top = pl.multiple_of(block * ROWS, ROWS)
        for z in range(depth):
            for c in range(chunks):
                field[z, c, pl.ds(pl.multiple_of(top + PAD, PAD), ROWS), :] = encode(
                    scores[z, pl.ds(top, ROWS), columns[c]], total
                )

    pl.semaphore_wait(barrier, n - 1)

    def exchange(send, recv, phase, step, side, part, arrival):
        rows = pl.ds(pl.multiple_of(part * (part_rows // 2), part_rows // 2), part_rows // 2)
        there = arrival if arrival is not None else 1 - side
        return pltpu.make_async_remote_copy(
            src_ref=send.at[phase, side, rows, :],
            dst_ref=recv.at[phase, there, rows, :],
            send_sem=send_sem.at[step, side, part],
            recv_sem=recv_sem.at[step, there, part],
            device_id=(me + (1 if side else -1),),
            device_id_type=pl.DeviceIdType.MESH,
        )

    def start(send, recv, phase, step, part):
        for side in range(2):

            @pl.when(has[side])
            def _():
                exchange(send, recv, phase, step, side, part, None).start()

    def finish(send, recv, phase, step, part):
        for side in range(2):

            @pl.when(has[side])
            def _():
                exchange(send, recv, phase, step, side, part, None).wait_send()
                exchange(send, recv, phase, step, side, part, side).wait_recv()

    def search(phase, part):
        place = spot(FINE)

        @pl.loop(0, part_rows // FINE)
        def _(block):
            top = pl.multiple_of(part * part_rows + block * FINE, FINE)
            here = pl.ds(top, FINE)
            wide = [
                spread(
                    lambda c, d: field[z, c, pl.ds(top + (PAD + d), FINE), :],
                    chunks, jnp.maximum, NONE, lane,
                )
                for z in range(depth)
            ]
            codes = ([], [])
            count = jnp.zeros((FINE, LANES), jnp.int32)
            for c in range(chunks):
                w = [wide[z][c] for z in range(depth)]
                low, high = jnp.maximum(w[0], w[1]), jnp.maximum(w[-1], w[-2])
                near[0, 0, c, here, :] = w[0]
                near[0, 1, c, here, :] = low
                near[1, 0, c, here, :] = high
                near[1, 1, c, here, :] = w[-1]
                own = jnp.zeros((FINE, LANES), jnp.int32)
                best = []
                for z in range(depth):
                    value = field[z, c, pl.ds(pl.multiple_of(top + PAD, PAD), FINE), :]
                    terms = {k: w[k] for k in range(max(z - 2, 0), min(z + 3, depth))}
                    if 0 in terms and 1 in terms:
                        terms[0] = low
                        del terms[1]
                    if depth - 1 in terms and depth - 2 in terms:
                        terms[depth - 1] = high
                        del terms[depth - 2]
                    is_best = value == functools.reduce(jnp.maximum, list(terms.values()))
                    if phase:
                        is_best = is_best & (value > NONE)
                    own = own | jnp.where(is_best, 4 << z, 0)
                    best.append(is_best)
                found[c, here, :] = own
                for side in range(2):
                    a, b = edge[side]
                    held_a = scores[a, here, columns[c]]
                    held_b = scores[b, here, columns[c]]
                    codes[side].append(
                        jnp.where(
                            best[a],
                            held_a * 8 + place,
                            jnp.where(best[b], held_b * 8 + (place + 4), -1),
                        )
                    )
                if phase:
                    for side in range(2):
                        for z in edge[side]:
                            count = count + jnp.where(best[z], lone[side], 0)
                    for z in range(2, depth - 2):
                        count = count + jnp.where(best[z], 1, 0)
            small = pl.ds(pl.multiple_of(top // 2, FINE // 2), FINE // 2)
            for side in range(2):
                for c, v in enumerate(pack(codes[side])):
                    cand_send[phase, side, small, columns[c]] = v
            if phase:
                tally[2, :FINE] += count

    def judge(phase, part):
        place = spot(ROWS)

        @pl.loop(0, part_rows // ROWS)
        def _(block):
            top = pl.multiple_of(part * part_rows + block * ROWS, ROWS)
            small = pl.ds(pl.multiple_of(top // 2, ROWS // 2), ROWS // 2)
            here = pl.ds(top, ROWS)
            halo = [jnp.zeros((ROWS, LANES), jnp.int32) for _ in range(chunks)]
            count = jnp.zeros((ROWS, LANES), jnp.int32)
            for side in range(2):
                codes = unpack(
                    [cand_recv[phase, side, small, columns[c]] for c in range(chunks // 2)]
                )
                verdicts = []
                for c, code in enumerate(codes):
                    where = code & 7
                    score = jnp.where(code < 0, NONE, encode(code >> 3, total))
                    low = (where == place) & (score > near[side, 0, c, here, :])
                    high = (where == place + 4) & (score > near[side, 1, c, here, :])
                    alive = jnp.where(low | high, 1, 0)
                    verdicts.append(alive)
                    if phase:
                        count = count + alive
                    else:
                        halo[c] = halo[c] | jnp.where(low, 1 << halo_bits[side][0], 0)
                        halo[c] = halo[c] | jnp.where(high, 1 << halo_bits[side][1], 0)
                for c, v in enumerate(pack(verdicts)):
                    resp_send[phase, side, small, columns[c]] = v.astype(
                        jnp.float32
                    ).astype(jnp.bfloat16)
            if phase:
                tally[2] += count
            else:
                for c in range(chunks):
                    bits[c, pl.ds(pl.multiple_of(top + PAD, PAD), ROWS), :] = halo[c]

    def confirmed(phase, top):
        small = pl.ds(pl.multiple_of(top // 2, ROWS // 2), ROWS // 2)
        own = [found[c, pl.ds(top, ROWS), :] for c in range(chunks)]
        for side in range(2):
            verdicts = unpack(
                [
                    resp_recv[phase, side, small, columns[c]].astype(jnp.float32)
                    for c in range(chunks // 2)
                ]
            )
            mask = (4 << edge[side][0]) | (4 << edge[side][1])
            own = [jnp.where(v > 0.5, o, o & ~mask) for v, o in zip(verdicts, own)]
        return own

    def settle(part):
        @pl.loop(0, part_rows // ROWS)
        def _(block):
            top = pl.multiple_of(part * part_rows + block * ROWS, ROWS)
            for c, own in enumerate(confirmed(0, top)):
                bits[c, pl.ds(pl.multiple_of(top + PAD, PAD), ROWS), :] |= own

    def remove(part):
        @pl.loop(0, part_rows // FINE)
        def _(block):
            top = pl.multiple_of(part * part_rows + block * FINE, FINE)
            centre = pl.ds(pl.multiple_of(top + PAD, PAD), FINE)
            reach = spread(
                lambda c, d: bits[c, pl.ds(top + (PAD + d), FINE), :],
                chunks, jnp.bitwise_or, 0, lane,
            )
            first, second = tally[0, :FINE], tally[1, :FINE]
            for c in range(chunks):
                roots = bits[c, centre, :]
                status = jnp.zeros((FINE, LANES), jnp.int32)
                for z in range(depth):
                    is_root = (roots & (4 << z)) != 0
                    covered = (reach[c] & (31 << z)) != 0
                    field[z, c, centre, :] = jnp.where(covered, NONE, field[z, c, centre, :])
                    status = status | jnp.where(
                        is_root, 1 << (2 * z), jnp.where(covered, 2 << (2 * z), 0)
                    )
                    first = first + jnp.where(is_root, 1, 0)
                    second = second + jnp.where(covered, 1, 0)
                packed_status[pl.ds(top, FINE), columns[c]] = status
            tally[0, :FINE] = first
            tally[1, :FINE] = second

    def offer(phase, part):
        search(phase, part)
        start(cand_send, cand_recv, phase, 2 * phase, part)

    def answer(phase, part):
        finish(cand_send, cand_recv, phase, 2 * phase, part)
        judge(phase, part)
        start(resp_send, resp_recv, phase, 2 * phase + 1, part)

    @pl.loop(0, PARTS)
    def _(part):
        offer(0, part)

    @pl.loop(0, PARTS)
    def _(part):
        answer(0, part)

    @pl.loop(0, PARTS + 2)
    def _(part):
        @pl.when(part < PARTS)
        def _():
            finish(resp_send, resp_recv, 0, 1, part)
            settle(part)

        @pl.when((part > 0) & (part <= PARTS))
        def _():
            remove(part - 1)

        @pl.when(part > 1)
        def _():
            offer(1, part - 2)

    @pl.loop(0, PARTS)
    def _(part):
        answer(1, part)

    roots, covered, late = (jnp.sum(tally[i]) for i in range(3))
    cells = depth * nx * ny
    column = lax.broadcasted_iota(jnp.int32, cnt_send.shape, 1)
    mine = jnp.where(
        column == 0,
        cells - roots,
        jnp.where(column == 1, cells - covered, cells - covered - late),
    )
    cnt_send[...] = mine

    def report(i):
        return pltpu.make_async_remote_copy(
            src_ref=cnt_send,
            dst_ref=cnt_recv.at[i],
            send_sem=cnt_send_sem.at[i],
            recv_sem=cnt_recv_sem.at[i],
            device_id=(lax.rem(me + i, n),),
            device_id_type=pl.DeviceIdType.MESH,
        )

    @pl.loop(1, n)
    def _(i):
        report(i).start()

    @pl.loop(0, PARTS)
    def _(part):
        finish(resp_send, resp_recv, 1, 3, part)

        @pl.loop(0, part_rows // ROWS)
        def _(block):
            top = pl.multiple_of(part * part_rows + block * ROWS, ROWS)
            for c, own in enumerate(confirmed(1, top)):
                status = packed_status[pl.ds(top, ROWS), columns[c]]
                for z in range(depth):
                    status = status | jnp.where((own & (4 << z)) != 0, 1 << (2 * z), 0)
                packed_status[pl.ds(top, ROWS), columns[c]] = status

    @pl.loop(1, n)
    def _(i):
        report(i).wait()

    cnt_recv[0] = mine
    counts[...] = jnp.sum(cnt_recv[...], axis=0)


def shards(scores):
    depth, nx, ny = scores.shape
    n = lax.axis_size(AXIS)
    vmem = pltpu.VMEM
    small = (nx // 2, ny // 2)
    chunks = ny // LANES
    packed_status, counts = pl.pallas_call(
        functools.partial(kernel, n),
        out_shape=(
            jax.ShapeDtypeStruct((nx, ny), jnp.int32),
            jax.ShapeDtypeStruct((8, 128), jnp.int32),
        ),
        in_specs=[pl.BlockSpec(memory_space=vmem)],
        out_specs=(pl.BlockSpec(memory_space=vmem),) * 2,
        scratch_shapes=[
            vmem((depth, chunks, nx + 2 * PAD, LANES), jnp.float32),
            vmem((2, 2, chunks, nx, LANES), jnp.float32),
            vmem((chunks, nx + 2 * PAD, LANES), jnp.int32),
            vmem((chunks, nx, LANES), jnp.int32),
            vmem((2, 2) + small, jnp.int32),
            vmem((2, 2) + small, jnp.int32),
            vmem((2, 2) + small, jnp.bfloat16),
            vmem((2, 2) + small, jnp.bfloat16),
            vmem((3, ROWS, LANES), jnp.int32),
            vmem((8, 128), jnp.int32),
            vmem((n, 8, 128), jnp.int32),
            pltpu.SemaphoreType.DMA((4, 2, PARTS)),
            pltpu.SemaphoreType.DMA((4, 2, PARTS)),
            pltpu.SemaphoreType.DMA((n,)),
            pltpu.SemaphoreType.DMA((n,)),
        ],
        compiler_params=pltpu.CompilerParams(
            collective_id=0, has_side_effects=True, vmem_limit_bytes=48 * 1024 * 1024
        ),
    )(scores)
    place = 2 * jnp.arange(depth, dtype=jnp.int32)[:, None, None]
    return (packed_status[None] >> place) & 3, counts[0, :3]


def solution(mesh):
    return jax.shard_map(
        shards,
        mesh=mesh,
        in_specs=(P(AXIS, None, None),),
        out_specs=(P(AXIS, None, None), P()),
        check_vma=False,
    )
```
